32 devices in a mesh: section: 4 (over y, x), ctx: 8 (over z, core).
Axes of the slice: x: 2, y: 2, z: 4, core: 2. Of those that a mesh axis runs over, the one named last changes fastest.
Arguments:
- queries: bfloat16 [4, 8, 1024, 512], P('section', None, 'ctx'), may hold values from -5 to 5
- keys: bfloat16 [4, 8, 1024, 128], P('section', None, 'ctx'), may hold values from -5 to 5
- values: bfloat16 [4, 8, 1024, 128], P('section', None, 'ctx'), may hold values from -6 to 6
- out_grad: bfloat16 [4, 1024, 512], P('section', 'ctx'), may hold values from -6 to 6
- stretch_ids: int32 [16], P('ctx'), may hold values from 0 to 15, as said below
- stash_slot: int32 [4], P('section'), may hold values from 0 to 7
Outputs:
- passed_grads: bfloat16 [4, 1024, 768], P('section', 'ctx')
The draws below stay inside these ranges and needn't reach their ends.
Inputs may be any that keep to these rules, and one draw needn't show every extreme that they name: `stretch_ids`: for each sequence, the entries of its 8 row blocks (two a block, blocks in order) are a permutation of 0 to 15 in which a block's two entries are some c and 15 - c, in either order.
All inputs are finite; a program needn't handle non-finite values.
Results may differ from the reference program's by a relative error of at most 0.035.
Values may be sent and summed in bfloat16 or wider, within the bound.
No kernel may reach another device: no remote copies, remote signals or barrier semaphores. Data moves between devices by JAX's collectives and lax.ppermute only.
A program may use at most 64 MiB of HBM per device.

```python
import math
import jax
import jax.numpy as jnp
from jax import lax

GROUP = 4
HEAD = 128
TOK_DEV = 128
SEQS = 1
MICRO = 8
HALF = 64
SPAN = 8
STRETCHES = 16
TOKENS = 1024
LENGTH = 1024
SECTIONS = 4
QW = 512


def draw_queries(key, part):
    shape = (SECTIONS, MICRO, TOKENS, GROUP * HEAD)
    return jax.random.truncated_normal(jax.random.fold_in(key, 7), -5.0, 5.0, shape, jnp.float32).astype(jnp.bfloat16)


def draw_keys(key, part):
    shape = (SECTIONS, MICRO, TOKENS, HEAD)
    return jax.random.truncated_normal(jax.random.fold_in(key, 17), -5.0, 5.0, shape, jnp.float32).astype(jnp.bfloat16)


def sequence_stretches(seq_key):
    order = jax.random.permutation(jax.random.fold_in(seq_key, 1), SPAN).astype(jnp.int32)
    flips = jax.random.randint(jax.random.fold_in(seq_key, 2), (SPAN,), 0, 2).astype(jnp.int32)
    mirror = (2 * SPAN - 1 - order).astype(jnp.int32)
    first = jnp.where(flips == 1, mirror, order)
    second = jnp.where(flips == 1, order, mirror)
    return jnp.stack([first, second], axis=1).astype(jnp.int32)


def draw_stretch_ids(key, part):
    seq_keys = jax.random.split(jax.random.fold_in(key, 11), SEQS)
    per_seq = jax.vmap(sequence_stretches)(seq_keys)
    return jnp.swapaxes(per_seq, 0, 1).reshape(STRETCHES).astype(jnp.int32)


def place_ends(entries, key, smallest, largest):
    spot = [jax.random.randint(jax.random.fold_in(key, axis), (), 0, length) for axis, length in enumerate(entries.shape)]
    main_axis = entries.shape.index(max(entries.shape))
    neighbour = spot[:main_axis] + [(spot[main_axis] + 1) % entries.shape[main_axis]] + spot[main_axis + 1:]
    return entries.at[tuple(spot)].set(smallest).at[tuple(neighbour)].set(largest)


def steps_of(own_key, shape, cuts, smallest, high):
    loudness, own = 1.0, jax.random.fold_in(own_key, 6)
    for axis_at, shards_of in cuts:
        draws = jnp.exp(jax.random.uniform(jax.random.fold_in(own, axis_at), (shards_of,), jnp.float32, smallest / len(cuts), high / len(cuts)))
        loudness = loudness * jnp.repeat(draws, shape[axis_at] // shards_of).reshape([-1 if axis == axis_at else 1 for axis in range(len(shape))])
    return loudness


def bell_draw(rng, extent, width, most, shards=(), kind=jnp.bfloat16):
    level = steps_of(rng, extent, shards, -0.22, 0.18) if shards else 1.0
    result = jax.random.normal(rng, extent, jnp.float32) * width * level
    return jnp.minimum(jnp.maximum(result, -most), most).astype(kind)


def setup_inputs(seed: int = 0) -> dict:
    splits = jax.random.split(jax.random.key(seed), 7)
    queries = draw_queries(jax.random.fold_in(splits[6], 71), 0)
    keys = draw_keys(jax.random.fold_in(splits[6], 71), 0)
    values = bell_draw(splits[2], (SECTIONS, MICRO, TOKENS, HEAD), 1.0, 6.0, ((0, 4), (2, 8)))
    out_grad = bell_draw(splits[3], (SECTIONS, TOKENS, QW), 1.0, 6.0, ((0, 4), (1, 8)))
    stretch_ids = draw_stretch_ids(jax.random.fold_in(splits[6], 71), 0)
    stash_slot = place_ends(jax.random.randint(splits[5], (SECTIONS,), 0, MICRO), jax.random.fold_in(splits[5], 1), 0, MICRO - 1).astype(jnp.int32)
    return dict(queries=queries, keys=keys, values=values, out_grad=out_grad, stretch_ids=stretch_ids, stash_slot=stash_slot)


def section_message(query_all, key_all, value_all, grad_all, token_place):
    softmax_scale = 1.0 / math.sqrt(HEAD)
    block_width = math.gcd(LENGTH, 256)
    blocks = LENGTH // block_width
    key_wide = key_all.astype(jnp.float32)
    value_wide = value_all.astype(jnp.float32)

    def one_block(sums_now, block_index):
        start = block_index * block_width
        query_rows = lax.dynamic_slice_in_dim(query_all, start, block_width, 0).astype(jnp.float32).reshape(block_width, GROUP, HEAD)
        grad_rows = lax.dynamic_slice_in_dim(grad_all, start, block_width, 0).astype(jnp.float32).reshape(block_width, GROUP, HEAD)
        query_place = lax.dynamic_slice_in_dim(token_place, start, block_width, 0)
        visible = token_place[None, None, :] <= query_place[:, None, None]
        scores = jnp.einsum('thd,cd->thc', query_rows, key_wide) * softmax_scale
        scores = jnp.where(visible, scores, -jnp.inf)
        row_top = lax.optimization_barrier(jnp.max(scores, axis=2, keepdims=True))
        log_total = row_top + jnp.log(lax.optimization_barrier(jnp.sum(jnp.exp(scores - row_top), axis=2, keepdims=True)))
        weights = jnp.exp(scores - log_total)
        probs_half = lax.optimization_barrier(weights.astype(jnp.bfloat16)).astype(jnp.float32)
        attention = jnp.einsum('thc,cd->thd', probs_half, value_wide)
        row_delta = lax.optimization_barrier(jnp.sum(grad_rows * attention, axis=2, keepdims=True))
        prob_grad = jnp.einsum('thd,cd->thc', grad_rows, value_wide)
        score_grad = lax.optimization_barrier((softmax_scale * weights * (prob_grad - row_delta)).astype(jnp.bfloat16)).astype(jnp.float32)
        query_grad = jnp.einsum('thc,cd->thd', score_grad, key_wide)
        key_grad = sums_now[0] + jnp.einsum('thc,thd->cd', score_grad, query_rows)
        value_grad = sums_now[1] + jnp.einsum('thc,thd->cd', probs_half, grad_rows)
        return ((key_grad, value_grad), query_grad.reshape(block_width, GROUP * HEAD))
    zero_rows = jnp.zeros((LENGTH, HEAD), jnp.float32)
    final_sums, query_grad = lax.scan(one_block, (zero_rows, zero_rows), jnp.arange(blocks, dtype=jnp.int32))
    query_grad = query_grad.reshape(LENGTH, GROUP * HEAD)
    return jnp.concatenate([query_grad, final_sums[0], final_sums[1]], axis=1).astype(jnp.bfloat16)

def regroup(array):
    tail = array.shape[1:]
    return jnp.swapaxes(array.reshape((SPAN, SEQS, TOK_DEV) + tail), 0, 1).reshape((SEQS, LENGTH) + tail)

def ungroup(array):
    tail = array.shape[2:]
    return jnp.swapaxes(array.reshape((SEQS, SPAN, TOK_DEV) + tail), 0, 1).reshape((TOKENS,) + tail)

def reference(queries, keys, values, out_grad, stretch_ids, stash_slot):
    row_ids = jnp.arange(TOKENS, dtype=jnp.int32)
    token_place = regroup(stretch_ids[row_ids // HALF] * HALF + row_ids % HALF)

    def per_section(section_index):
        stash_index = stash_slot[section_index]
        query_seq = regroup(queries[section_index, stash_index])
        key_seq = regroup(keys[section_index, stash_index])
        value_seq = regroup(values[section_index, stash_index])
        grad_seq = regroup(out_grad[section_index])

        def per_sequence(seq_index):
            return section_message(query_seq[seq_index], key_seq[seq_index], value_seq[seq_index], grad_seq[seq_index], token_place[seq_index])
        return ungroup(lax.map(per_sequence, jnp.arange(SEQS, dtype=jnp.int32)))
    messages = lax.map(per_section, jnp.arange(SECTIONS, dtype=jnp.int32))
    return jnp.roll(messages, -1, axis=0)
```

```python
import functools
import math

import jax
import jax.numpy as jnp
from jax import lax
from jax.experimental import pallas as pl
from jax.experimental.pallas import tpu as pltpu
from jax.sharding import PartitionSpec as P


MASKED = -1e30
FLOOR = -1e29
ID_ROWS = 16
LOG2E = 1.4426950408889634
VMEM_GRANT = 24 * 1024 * 1024


def vmem_spec():
    return pl.BlockSpec(memory_space=pltpu.VMEM)


def any_spec():
    return pl.BlockSpec(memory_space=pl.ANY)


def smem_spec():
    return pl.BlockSpec(memory_space=pltpu.SMEM)


def partner_swap(value, count):
    return lax.ppermute(value, "ctx", [(i, i ^ 1) for i in range(count)])


def chip_pairs(count, step):
    chips = count // 2
    if chips & (chips - 1) == 0:
        target = [z ^ step for z in range(chips)]
    else:
        target = [(z + step) % chips for z in range(chips)]
    return [(2 * z + k, 2 * target[z] + k) for z in range(chips) for k in range(2)]


def chip_send(value, count, step):
    return lax.ppermute(value, "ctx", chip_pairs(count, step))


def chip_return(value, count, step):
    return lax.ppermute(value, "ctx", [(b, a) for a, b in chip_pairs(count, step)])


def fetch_kernel(slot_ref, ids_ref, query_ref, key_ref, value_ref, grad_ref, kv_ref, qg_ref, sems):
    rows, head = key_ref.shape[2:]
    group = query_ref.shape[3] // head
    slot = slot_ref[0]
    copies = [
        pltpu.make_async_copy(key_ref.at[0, slot], kv_ref.at[0:rows, 0:head], sems.at[0]),
        pltpu.make_async_copy(value_ref.at[0, slot], kv_ref.at[0:rows, head : 2 * head], sems.at[1]),
    ]
    for h in range(group):
        cols = slice(h * head, (h + 1) * head)
        copies.append(
            pltpu.make_async_copy(
                query_ref.at[0, slot, :, cols], qg_ref.at[h * rows : (h + 1) * rows], sems.at[2 + 2 * h]
            )
        )
        copies.append(
            pltpu.make_async_copy(
                grad_ref.at[0, :, cols],
                qg_ref.at[(group + h) * rows : (group + h + 1) * rows],
                sems.at[3 + 2 * h],
            )
        )
    for copy in copies:
        copy.start()
    half = ID_ROWS // 2
    row = lax.broadcasted_iota(jnp.int32, (ID_ROWS, 2 * head), 0)
    ids = jnp.where(row < half, ids_ref[0], ids_ref[1]).astype(jnp.float32).astype(jnp.bfloat16)
    kv_ref[rows : rows + ID_ROWS, :] = ids
    qg_ref[2 * group * rows : 2 * group * rows + ID_ROWS, :] = ids[:, 0:head]
    for copy in copies:
        copy.wait()


def id_lines(ref, start, width):
    half = ID_ROWS // 2
    lines = ref[start : start + ID_ROWS, 0:width].astype(jnp.float32)
    return lines[0:1], lines[half : half + 1]


def lane_positions(qg_ref, group, rows, head):
    stretch = rows // 2
    first, second = id_lines(qg_ref, 2 * group * rows, head)
    lane = lax.broadcasted_iota(jnp.int32, (1, rows), 1)
    base = jnp.where(lane < stretch, first, second) * stretch
    offset = jnp.where(lane < stretch, lane, lane - stretch).astype(jnp.float32)
    one_head = base + offset
    return jnp.concatenate([one_head] * group, axis=1)


def dot_nt(a, b):
    return lax.dot_general(a, b, (((1,), (1,)), ((), ())), preferred_element_type=jnp.float32)


def dot_nn(a, b):
    return lax.dot_general(a, b, (((1,), (0,)), ((), ())), preferred_element_type=jnp.float32)


def dot_tn(a, b):
    return lax.dot_general(a, b, (((0,), (0,)), ((), ())), preferred_element_type=jnp.float32)


def score_kernel(blocks, group, rows, head, *refs):
    qg_refs = refs[0:2]
    kv_refs = refs[2 : 2 + blocks]
    exp_ref, dprob_ref, stat_ref = refs[2 + blocks :]
    width = group * rows
    stretch = rows // 2
    scale = LOG2E / math.sqrt(head)
    in_stretch = lax.broadcasted_iota(jnp.int32, (stretch, 1), 0).astype(jnp.float32)
    for b in range(2):
        lanes = slice(b * width, (b + 1) * width)
        place = lane_positions(qg_refs[b], group, rows, head)
        query = qg_refs[b][0:width, :]
        grad = qg_refs[b][width : 2 * width, :]
        top = jnp.full((1, width), FLOOR, jnp.float32)
        for j in range(blocks):
            scores = dot_nt(kv_refs[j][0:rows, 0:head], query) * scale
            ids = id_lines(kv_refs[j], rows, head)
            for part in range(2):
                limit = place - stretch * jnp.concatenate([ids[part]] * group, axis=1)
                seen = in_stretch <= limit
                piece = jnp.where(seen, scores[part * stretch : (part + 1) * stretch], MASKED)
                start = j * rows + part * stretch
                exp_ref[start : start + stretch, lanes] = piece
                top = jnp.maximum(top, jnp.max(piece, axis=0, keepdims=True))
        total = jnp.zeros((1, width), jnp.float32)
        mixed = jnp.zeros((1, width), jnp.float32)
        for j in range(blocks):
            span = slice(j * rows, (j + 1) * rows)
            raised = jnp.exp2(exp_ref[span, lanes] - top)
            dprob = dot_nt(kv_refs[j][0:rows, head : 2 * head], grad)
            exp_ref[span, lanes] = raised
            dprob_ref[span, lanes] = dprob
            total = total + jnp.sum(raised, axis=0, keepdims=True)
            mixed = mixed + jnp.sum(raised * dprob, axis=0, keepdims=True)
        stat_ref[0:1, lanes] = top
        stat_ref[1:2, lanes] = total
        stat_ref[2:3, lanes] = mixed
        stat_ref[3:8, lanes] = jnp.zeros((5, width), jnp.float32)


def grad_kernel(blocks, group, rows, head, *refs):
    exp_ref, dprob_ref, stat_ref, other_ref = refs[0:4]
    qg_refs = refs[4:6]
    kv_refs = refs[6 : 6 + blocks]
    dkv_refs = refs[6 + blocks : 6 + 2 * blocks]
    dq_refs = refs[6 + 2 * blocks : 8 + 2 * blocks]
    width = group * rows
    scale = 1.0 / math.sqrt(head)
    fade, delta = [], []
    for b in range(2):
        lanes = slice(b * width, (b + 1) * width)
        swapped = slice((1 - b) * width, (2 - b) * width)
        top, total, mixed = (stat_ref[i : i + 1, lanes] for i in range(3))
        top_o, total_o, mixed_o = (other_ref[i : i + 1, swapped] for i in range(3))
        high = jnp.maximum(top, top_o)
        own, other = jnp.exp2(top - high), jnp.exp2(top_o - high)
        inverse = 1.0 / (total * own + total_o * other)
        fade.append(own * inverse)
        delta.append((mixed * own + mixed_o * other) * inverse)
    dq = [None, None]
    for j in range(blocks):
        span = slice(j * rows, (j + 1) * rows)
        key = kv_refs[j][0:rows, 0:head]
        dk = dv = None
        for b in range(2):
            lanes = slice(b * width, (b + 1) * width)
            probs = exp_ref[span, lanes] * fade[b]
            dscore = (probs * (dprob_ref[span, lanes] - delta[b])).astype(jnp.bfloat16)
            probs = probs.astype(jnp.bfloat16)
            query = qg_refs[b][0:width, :]
            grad = qg_refs[b][width : 2 * width, :]
            dk_part, dv_part = dot_nn(dscore, query), dot_nn(probs, grad)
            dq_part = dot_tn(key, dscore)
            dk = dk_part if dk is None else dk + dk_part
            dv = dv_part if dv is None else dv + dv_part
            dq[b] = dq_part if dq[b] is None else dq[b] + dq_part
        dkv_refs[j][:, 0:head] = (dk * scale).astype(jnp.bfloat16)
        dkv_refs[j][:, head : 2 * head] = dv.astype(jnp.bfloat16)
    for b in range(2):
        for h in range(group):
            piece = jnp.transpose(dq[b][:, h * rows : (h + 1) * rows]) * scale
            dq_refs[b][:, h * head : (h + 1) * head] = piece.astype(dq_refs[b].dtype)


def params():
    return pltpu.CompilerParams(vmem_limit_bytes=VMEM_GRANT)


def per_device(queries, keys, values, out_grad, stretch_ids, stash_slot):
    rows, head = keys.shape[2:]
    group = queries.shape[3] // head
    width = group * rows
    count = lax.axis_size("ctx")
    blocks = count // 2
    sections = lax.axis_size("section")

    kv, qg = pl.pallas_call(
        fetch_kernel,
        out_shape=(
            jax.ShapeDtypeStruct((rows + ID_ROWS, 2 * head), jnp.bfloat16),
            jax.ShapeDtypeStruct((2 * width + ID_ROWS, head), jnp.bfloat16),
        ),
        in_specs=[smem_spec(), smem_spec(), any_spec(), any_spec(), any_spec(), any_spec()],
        out_specs=(vmem_spec(), vmem_spec()),
        scratch_shapes=[pltpu.SemaphoreType.DMA((2 + 2 * group,))],
        compiler_params=params(),
        name="fetch",
    )(stash_slot, stretch_ids, queries, keys, values, out_grad)

    kv_blocks = [kv] + [chip_send(kv, count, j) for j in range(1, blocks)]
    qg_other = partner_swap(qg, count)
    keys_here = blocks * rows
    raised, dprob, stats = pl.pallas_call(
        functools.partial(score_kernel, blocks, group, rows, head),
        out_shape=(
            jax.ShapeDtypeStruct((keys_here, 2 * width), jnp.float32),
            jax.ShapeDtypeStruct((keys_here, 2 * width), jnp.float32),
            jax.ShapeDtypeStruct((8, 2 * width), jnp.float32),
        ),
        in_specs=[vmem_spec()] * (2 + blocks),
        out_specs=(vmem_spec(),) * 3,
        compiler_params=params(),
        name="scores",
    )(qg, qg_other, *kv_blocks)
    stats_other = partner_swap(stats, count)
    outs = pl.pallas_call(
        functools.partial(grad_kernel, blocks, group, rows, head),
        out_shape=tuple(jax.ShapeDtypeStruct((rows, 2 * head), jnp.bfloat16) for _ in range(blocks))
        + (
            jax.ShapeDtypeStruct((rows, group * head), jnp.float32),
            jax.ShapeDtypeStruct((rows, group * head), jnp.bfloat16),
        ),
        in_specs=[vmem_spec()] * (6 + blocks),
        out_specs=(vmem_spec(),) * (blocks + 2),
        compiler_params=params(),
        name="grads",
    )(raised, dprob, stats, stats_other, qg, qg_other, *kv_blocks)
    dkv_blocks, (dq_own, dq_other) = outs[:blocks], outs[blocks:]
    back = [(i, (i - 1) % sections) for i in range(sections)]
    dkv = dkv_blocks[0].astype(jnp.float32)
    for j in range(1, blocks):
        dkv = dkv + chip_return(dkv_blocks[j], count, j).astype(jnp.float32)
    dq = dq_own + partner_swap(dq_other, count).astype(jnp.float32)
    dq_message = lax.ppermute(dq.astype(jnp.bfloat16), "section", back)
    dkv_message = lax.ppermute(dkv.astype(jnp.bfloat16), "section", back)
    return jnp.concatenate([dq_message, dkv_message], axis=1)[None]


def solution(mesh):
    in_specs = (
        P("section", None, "ctx", None),
        P("section", None, "ctx", None),
        P("section", None, "ctx", None),
        P("section", "ctx", None),
        P("ctx"),
        P("section"),
    )
    out_specs = P("section", "ctx", None)
    return jax.shard_map(
        per_device, mesh=mesh, in_specs=in_specs, out_specs=out_specs, check_vma=False
    )
```

```python
import functools
import math

import jax
import jax.numpy as jnp
from jax import lax
from jax.experimental import pallas as pl
from jax.experimental.pallas import tpu as pltpu
from jax.sharding import PartitionSpec as P


MASKED = -1e30
FLOOR = -1e29
ID_ROWS = 8
LOG2E = 1.4426950408889634
VMEM_GRANT = 8 * 1024 * 1024


def vmem_spec():
    return pl.BlockSpec(memory_space=pltpu.VMEM)


def in_hbm(value):
    return pltpu.with_memory_space_constraint(value, pltpu.HBM)


def hbm_spec():
    return pl.BlockSpec(memory_space=pltpu.HBM)


def partner_swap(value, count):
    return lax.ppermute(value, "ctx", [(i, i ^ 1) for i in range(count)])


def chip_pairs(count, step):
    chips = count // 2
    if chips & (chips - 1) == 0:
        target = [z ^ step for z in range(chips)]
    else:
        target = [(z + step) % chips for z in range(chips)]
    return [(2 * z + k, 2 * target[z] + k) for z in range(chips) for k in range(2)]


def chip_send(value, count, step):
    return lax.ppermute(value, "ctx", chip_pairs(count, step))


def chip_return(value, count, step):
    return lax.ppermute(value, "ctx", [(b, a) for a, b in chip_pairs(count, step)])


def fetch_kernel(slot_ref, ids_ref, query_ref, key_ref, value_ref, grad_ref, kv_ref, qg_ref, ids, sems):
    rows, head = key_ref.shape[2:]
    group = query_ref.shape[3] // head
    slot = slot_ref[0]
    ids_copy = pltpu.make_async_copy(ids_ref, ids, sems.at[0])
    copies = [
        pltpu.make_async_copy(key_ref.at[0, slot], kv_ref.at[0:rows, 0:head], sems.at[1]),
        pltpu.make_async_copy(value_ref.at[0, slot], kv_ref.at[0:rows, head : 2 * head], sems.at[2]),
    ]
    for h in range(group):
        cols = slice(h * head, (h + 1) * head)
        query_to = qg_ref.at[h * rows : (h + 1) * rows]
        grad_to = qg_ref.at[(group + h) * rows : (group + h + 1) * rows]
        copies.append(
            pltpu.make_async_copy(query_ref.at[0, slot, :, cols], query_to, sems.at[3 + 2 * h])
        )
        copies.append(pltpu.make_async_copy(grad_ref.at[0, :, cols], grad_to, sems.at[4 + 2 * h]))
    ids_copy.start()
    for copy in copies:
        copy.start()
    ids_copy.wait()
    half = ID_ROWS // 2
    row = lax.broadcasted_iota(jnp.int32, (ID_ROWS, 2 * head), 0)
    lines = jnp.where(row < half, ids[0], ids[1]).astype(jnp.float32).astype(jnp.bfloat16)
    kv_ref[rows : rows + ID_ROWS, :] = lines
    qg_ref[2 * group * rows : 2 * group * rows + ID_ROWS, :] = lines[:, 0:head]
    for copy in copies:
        copy.wait()


def id_lines(ref, start, width):
    half = ID_ROWS // 2
    lines = ref[start : start + ID_ROWS, 0:width].astype(jnp.float32)
    return lines[0:1], lines[half : half + 1]


def lane_positions(qg_ref, group, rows, head):
    stretch = rows // 2
    first, second = id_lines(qg_ref, 2 * group * rows, head)
    lane = lax.broadcasted_iota(jnp.int32, (1, rows), 1)
    base = jnp.where(lane < stretch, first, second) * stretch
    offset = jnp.where(lane < stretch, lane, lane - stretch).astype(jnp.float32)
    one_head = base + offset
    return jnp.concatenate([one_head] * group, axis=1)


def dot_nt(a, b):
    return lax.dot_general(a, b, (((1,), (1,)), ((), ())), preferred_element_type=jnp.float32)


def dot_nn(a, b):
    return lax.dot_general(a, b, (((1,), (0,)), ((), ())), preferred_element_type=jnp.float32)


def dot_tn(a, b):
    return lax.dot_general(a, b, (((0,), (0,)), ((), ())), preferred_element_type=jnp.float32)


def score_kernel(group, rows, head, earlier, *refs):
    qg_refs, kv_ref = refs[0:2], refs[2]
    earlier_refs = refs[3 : 3 + earlier]
    exp_ref, dprob_ref, stat_ref = refs[3 + earlier : 6 + earlier]
    width = group * rows
    stretch = rows // 2
    scale = LOG2E / math.sqrt(head)
    in_stretch = lax.broadcasted_iota(jnp.int32, (stretch, 1), 0).astype(jnp.float32)
    ids = id_lines(kv_ref, rows, head)
    key, value = kv_ref[0:rows, 0:head], kv_ref[0:rows, head : 2 * head]
    for b in range(2):
        lanes = slice(b * width, (b + 1) * width)
        place = lane_positions(qg_refs[b], group, rows, head)
        query = qg_refs[b][0:width, :]
        grad = qg_refs[b][width : 2 * width, :]
        scores = dot_nt(key, query) * scale
        dprob = dot_nt(value, grad)
        pieces = []
        for part in range(2):
            limit = place - stretch * jnp.concatenate([ids[part]] * group, axis=1)
            piece = scores[part * stretch : (part + 1) * stretch]
            pieces.append(jnp.where(in_stretch <= limit, piece, MASKED))
        scores = jnp.concatenate(pieces, axis=0)
        top = jnp.maximum(jnp.max(scores, axis=0, keepdims=True), FLOOR)
        raised = jnp.exp2(scores - top)
        exp_ref[:, lanes] = raised
        dprob_ref[:, lanes] = dprob
        stat_ref[0:1, lanes] = top
        stat_ref[1:2, lanes] = jnp.sum(raised, axis=0, keepdims=True)
        stat_ref[2:3, lanes] = jnp.sum(raised * dprob, axis=0, keepdims=True)
        stat_ref[3:8, lanes] = jnp.zeros((5, width), jnp.float32)
    if earlier:
        merged_ref = refs[6 + earlier]
        parts = [ref[...] for ref in earlier_refs] + [stat_ref[...]]
        top = functools.reduce(jnp.maximum, [part[0:1] for part in parts])
        fades = [jnp.exp2(part[0:1] - top) for part in parts]
        merged_ref[0:1, :] = top
        merged_ref[1:2, :] = sum(part[1:2] * fade for part, fade in zip(parts, fades))
        merged_ref[2:3, :] = sum(part[2:3] * fade for part, fade in zip(parts, fades))
        merged_ref[3:8, :] = jnp.zeros((5, 2 * width), jnp.float32)


def block_grads(group, rows, head, refs, dkv_ref, dscore_ref):
    exp_ref, dprob_ref, stat_ref, merged_ref, other_ref = refs[0:5]
    qg_refs = refs[5:7]
    width = group * rows
    dk = dv = None
    for b in range(2):
        lanes = slice(b * width, (b + 1) * width)
        swapped = slice((1 - b) * width, (2 - b) * width)
        top, total, mixed = (merged_ref[i : i + 1, lanes] for i in range(3))
        top_o, total_o, mixed_o = (other_ref[i : i + 1, swapped] for i in range(3))
        high = jnp.maximum(top, top_o)
        own, other = jnp.exp2(top - high), jnp.exp2(top_o - high)
        inverse = 1.0 / (total * own + total_o * other)
        delta = (mixed * own + mixed_o * other) * inverse
        fade = jnp.exp2(stat_ref[0:1, lanes] - high) * inverse
        probs = exp_ref[:, lanes] * fade
        dscore = (probs * (dprob_ref[:, lanes] - delta)).astype(jnp.bfloat16)
        dscore_ref[:, lanes] = dscore
        dk_part = dot_nn(dscore, qg_refs[b][0:width, :])
        dv_part = dot_nn(probs.astype(jnp.bfloat16), qg_refs[b][width : 2 * width, :])
        dk = dk_part if dk is None else dk + dk_part
        dv = dv_part if dv is None else dv + dv_part
    dkv_ref[:, 0:head] = (dk * (1.0 / math.sqrt(head))).astype(dkv_ref.dtype)
    dkv_ref[:, head : 2 * head] = dv.astype(dkv_ref.dtype)


def far_grad_kernel(group, rows, head, *refs):
    block_grads(group, rows, head, refs[0:7], refs[7], refs[8])


def near_grad_kernel(blocks, group, rows, head, *refs):
    kv_refs = refs[7 : 7 + blocks]
    dscore_refs = refs[7 + blocks : 6 + 2 * blocks]
    dkv_ref, dq_own_ref, dq_other_ref, dscore_ref = refs[6 + 2 * blocks :]
    width = group * rows
    scale = 1.0 / math.sqrt(head)
    block_grads(group, rows, head, refs[0:7], dkv_ref, dscore_ref)
    for b, dq_ref in enumerate((dq_own_ref, dq_other_ref)):
        lanes = slice(b * width, (b + 1) * width)
        dq = None
        for kv_ref, ref in zip(kv_refs, (dscore_ref,) + tuple(dscore_refs)):
            part = dot_tn(kv_ref[0:rows, 0:head], ref[:, lanes])
            dq = part if dq is None else dq + part
        for h in range(group):
            piece = jnp.transpose(dq[:, h * rows : (h + 1) * rows]) * scale
            dq_ref[:, h * head : (h + 1) * head] = piece.astype(dq_ref.dtype)


def params():
    return pltpu.CompilerParams(vmem_limit_bytes=VMEM_GRANT)


def per_device(queries, keys, values, out_grad, stretch_ids, stash_slot):
    rows, head = keys.shape[2:]
    group = queries.shape[3] // head
    width = group * rows
    count = lax.axis_size("ctx")
    blocks = count // 2
    sections = lax.axis_size("section")

    kv, qg = pl.pallas_call(
        fetch_kernel,
        out_shape=(
            jax.ShapeDtypeStruct((rows + ID_ROWS, 2 * head), jnp.bfloat16),
            jax.ShapeDtypeStruct((2 * width + ID_ROWS, head), jnp.bfloat16),
        ),
        in_specs=[pl.BlockSpec(memory_space=pltpu.SMEM)] + [hbm_spec()] * 5,
        out_specs=(vmem_spec(), vmem_spec()),
        scratch_shapes=[
            pltpu.SMEM(stretch_ids.shape, jnp.int32),
            pltpu.SemaphoreType.DMA((3 + 2 * group,)),
        ],
        compiler_params=params(),
        name="fetch",
    )(stash_slot, *(in_hbm(x) for x in (stretch_ids, queries, keys, values, out_grad)))

    steps = send_order(count)
    arrivals = arrival_order(count)
    kv_blocks = {0: kv}
    for j in steps:
        kv_blocks[j] = chip_send(kv, count, j)
    qg_other = partner_swap(qg, count)

    square = jax.ShapeDtypeStruct((rows, 2 * width), jnp.float32)
    lines = jax.ShapeDtypeStruct((8, 2 * width), jnp.float32)
    scored = {}
    for j in [0] + arrivals:
        last = j == arrivals[-1]
        earlier = [scored[i][2] for i in scored] if last else []
        scored[j] = pl.pallas_call(
            functools.partial(score_kernel, group, rows, head, len(earlier)),
            out_shape=(square, square, lines) + ((lines,) if last else ()),
            in_specs=[vmem_spec()] * (3 + len(earlier)),
            out_specs=(vmem_spec(),) * (4 if last else 3),
            compiler_params=params(),
        )(qg, qg_other, kv_blocks[j], *earlier)
    merged = scored[arrivals[-1]][3]
    merged_other = partner_swap(merged, count)

    dkv_shape = jax.ShapeDtypeStruct((rows, 2 * head), jnp.bfloat16)
    half_square = jax.ShapeDtypeStruct((rows, 2 * width), jnp.bfloat16)
    returned, dscores = {}, {}
    for j in steps:
        dkv_part, dscores[j] = pl.pallas_call(
            functools.partial(far_grad_kernel, group, rows, head),
            out_shape=(dkv_shape, half_square),
            in_specs=[vmem_spec()] * 7,
            out_specs=(vmem_spec(),) * 2,
            compiler_params=params(),
        )(*scored[j][0:3], merged, merged_other, qg, qg_other)
        returned[j] = chip_return(dkv_part, count, j)
    dkv_own, dq_own, dq_other = pl.pallas_call(
        functools.partial(near_grad_kernel, blocks, group, rows, head),
        out_shape=(
            jax.ShapeDtypeStruct((rows, 2 * head), jnp.float32),
            jax.ShapeDtypeStruct((rows, group * head), jnp.float32),
            jax.ShapeDtypeStruct((rows, group * head), jnp.bfloat16),
        ),
        in_specs=[vmem_spec()] * (6 + 2 * blocks),
        out_specs=(vmem_spec(),) * 3,
        scratch_shapes=[pltpu.VMEM((rows, 2 * width), jnp.bfloat16)],
        compiler_params=params(),
        name="grads0",
    )(
        *scored[0][0:3],
        merged,
        merged_other,
        qg,
        qg_other,
        kv,
        *(kv_blocks[j] for j in steps),
        *(dscores[j] for j in steps),
    )
    back = [(i, (i - 1) % sections) for i in range(sections)]
    dq_swapped = partner_swap(dq_other, count)
    dq = (dq_own + dq_swapped.astype(jnp.float32)).astype(jnp.bfloat16)
    dq_message = lax.ppermute(dq, "section", back)
    dkv = dkv_own
    for j in steps:
        dkv = dkv + returned[j].astype(jnp.float32)
    dkv_message = lax.ppermute(dkv.astype(jnp.bfloat16), "section", back)
    return jnp.concatenate([dq_message, dkv_message], axis=1)[None]


def send_order(count):
    return list(reversed(range(1, count // 2)))


def arrival_order(count):
    half = count // 4
    return [j for j in send_order(count) if j != half] + [half]


def solution(mesh):
    in_specs = (
        P("section", None, "ctx", None),
        P("section", None, "ctx", None),
        P("section", None, "ctx", None),
        P("section", "ctx", None),
        P("ctx"),
        P("section"),
    )
    out_specs = P("section", "ctx", None)

    return jax.shard_map(
        per_device, mesh=mesh, in_specs=in_specs, out_specs=out_specs, check_vma=False
    )
```

```python
import functools
import math

import jax
import jax.numpy as jnp
from jax import lax
from jax.experimental import pallas as pl
from jax.experimental.pallas import tpu as pltpu
from jax.sharding import PartitionSpec as P


MASKED = -1e30
FLOOR = -1e29
ID_ROWS = 8
LOG2E = 1.4426950408889634
VMEM_GRANT = 8 * 1024 * 1024


def vmem_spec():
    return pl.BlockSpec(memory_space=pltpu.VMEM)


def in_hbm(value):
    return pltpu.with_memory_space_constraint(value, pltpu.HBM)


def hbm_spec():
    return pl.BlockSpec(memory_space=pltpu.HBM)


def partner_swap(value, count):
    return lax.ppermute(value, "ctx", [(i, i ^ 1) for i in range(count)])


def chip_pairs(count, step):
    chips = count // 2
    if chips & (chips - 1) == 0:
        target = [z ^ step for z in range(chips)]
    else:
        target = [(z + step) % chips for z in range(chips)]
    return [(2 * z + k, 2 * target[z] + k) for z in range(chips) for k in range(2)]


def chip_send(value, count, step):
    return lax.ppermute(value, "ctx", chip_pairs(count, step))


def chip_return(value, count, step):
    return lax.ppermute(value, "ctx", [(b, a) for a, b in chip_pairs(count, step)])


def id_block(ids_ref, head):
    row = lax.broadcasted_iota(jnp.int32, (ID_ROWS, head), 0)
    chosen = jnp.where(row < ID_ROWS // 2, ids_ref[0], ids_ref[1])
    return chosen.astype(jnp.float32).astype(jnp.bfloat16)


def fetch_kv_kernel(slot_ref, ids_ref, key_ref, value_ref, kv_ref, ids, sems):
    rows, head = key_ref.shape[2:]
    slot = slot_ref[0]
    copies = [
        pltpu.make_async_copy(key_ref.at[0, slot], kv_ref.at[0:rows], sems.at[0]),
        pltpu.make_async_copy(value_ref.at[0, slot], kv_ref.at[rows : 2 * rows], sems.at[1]),
    ]
    ids_copy = pltpu.make_async_copy(ids_ref, ids, sems.at[2])
    ids_copy.start()
    for copy in copies:
        copy.start()
    ids_copy.wait()
    kv_ref[2 * rows : 2 * rows + ID_ROWS, :] = id_block(ids, head)
    for copy in copies:
        copy.wait()


def fetch_qg_kernel(slot_ref, query_ref, grad_ref, kv_ref, qg_ref, sems):
    rows, width = query_ref.shape[2:]
    head = kv_ref.shape[1]
    group = width // head
    slot = slot_ref[0]
    copies = []
    for h in range(group):
        cols = slice(h * head, (h + 1) * head)
        query_to = qg_ref.at[h * rows : (h + 1) * rows]
        grad_to = qg_ref.at[(group + h) * rows : (group + h + 1) * rows]
        copies.append(
            pltpu.make_async_copy(query_ref.at[0, slot, :, cols], query_to, sems.at[2 * h])
        )
        copies.append(pltpu.make_async_copy(grad_ref.at[0, :, cols], grad_to, sems.at[2 * h + 1]))
    for copy in copies:
        copy.start()
    last = 2 * group * rows
    qg_ref[last : last + ID_ROWS, :] = kv_ref[2 * rows : 2 * rows + ID_ROWS, :]
    for copy in copies:
        copy.wait()


def write_dq_kernel(dq_ref, out_ref, sem):
    copy = pltpu.make_async_copy(dq_ref, out_ref.at[0, :, 0 : dq_ref.shape[1]], sem)
    copy.start()
    copy.wait()


def write_dkv_kernel(filled_ref, dkv_ref, out_ref, sem):
    start = out_ref.shape[2] - dkv_ref.shape[1]
    copy = pltpu.make_async_copy(dkv_ref, out_ref.at[0, :, start : out_ref.shape[2]], sem)
    copy.start()
    copy.wait()


def id_lines(ref, start, width):
    half = ID_ROWS // 2
    lines = ref[start : start + ID_ROWS, 0:width].astype(jnp.float32)
    return lines[0:1], lines[half : half + 1]


def lane_positions(qg_ref, group, rows, head):
    stretch = rows // 2
    first, second = id_lines(qg_ref, 2 * group * rows, head)
    lane = lax.broadcasted_iota(jnp.int32, (1, rows), 1)
    base = jnp.where(lane < stretch, first, second) * stretch
    offset = jnp.where(lane < stretch, lane, lane - stretch).astype(jnp.float32)
    one_head = base + offset
    return jnp.concatenate([one_head] * group, axis=1)


def dot_nt(a, b):
    return lax.dot_general(a, b, (((1,), (1,)), ((), ())), preferred_element_type=jnp.float32)


def dot_nn(a, b):
    return lax.dot_general(a, b, (((1,), (0,)), ((), ())), preferred_element_type=jnp.float32)


def dot_tn(a, b):
    return lax.dot_general(a, b, (((0,), (0,)), ((), ())), preferred_element_type=jnp.float32)


def score_kernel(group, rows, head, earlier, *refs):
    qg_refs, kv_ref = refs[0:2], refs[2]
    earlier_refs = refs[3 : 3 + earlier]
    exp_ref, dprob_ref, stat_ref = refs[3 + earlier : 6 + earlier]
    width = group * rows
    stretch = rows // 2
    scale = LOG2E / math.sqrt(head)
    in_stretch = lax.broadcasted_iota(jnp.int32, (stretch, 1), 0).astype(jnp.float32)
    ids = id_lines(kv_ref, 2 * rows, head)
    key, value = kv_ref[0:rows, :], kv_ref[rows : 2 * rows, :]
    for b in range(2):
        lanes = slice(b * width, (b + 1) * width)
        place = lane_positions(qg_refs[b], group, rows, head)
        query = qg_refs[b][0:width, :]
        grad = qg_refs[b][width : 2 * width, :]
        scores = dot_nt(key, query) * scale
        dprob = dot_nt(value, grad)
        pieces = []
        for part in range(2):
            limit = place - stretch * jnp.concatenate([ids[part]] * group, axis=1)
            piece = scores[part * stretch : (part + 1) * stretch]
            pieces.append(jnp.where(in_stretch <= limit, piece, MASKED))
        scores = jnp.concatenate(pieces, axis=0)
        top = jnp.maximum(jnp.max(scores, axis=0, keepdims=True), FLOOR)
        raised = jnp.exp2(scores - top)
        exp_ref[:, lanes] = raised
        dprob_ref[:, lanes] = dprob
        stat_ref[0:1, lanes] = top
        stat_ref[1:2, lanes] = jnp.sum(raised, axis=0, keepdims=True)
        stat_ref[2:3, lanes] = jnp.sum(raised * dprob, axis=0, keepdims=True)
        stat_ref[3:8, lanes] = jnp.zeros((5, width), jnp.float32)
    if earlier:
        merged_ref = refs[6 + earlier]
        parts = [ref[...] for ref in earlier_refs] + [stat_ref[...]]
        top = functools.reduce(jnp.maximum, [part[0:1] for part in parts])
        fades = [jnp.exp2(part[0:1] - top) for part in parts]
        merged_ref[0:1, :] = top
        merged_ref[1:2, :] = sum(part[1:2] * fade for part, fade in zip(parts, fades))
        merged_ref[2:3, :] = sum(part[2:3] * fade for part, fade in zip(parts, fades))
        merged_ref[3:8, :] = jnp.zeros((5, 2 * width), jnp.float32)


def half_weights(refs, lanes, swapped):
    exp_ref, dprob_ref, stat_ref, merged_ref, other_ref = refs
    top, total, mixed = (merged_ref[i : i + 1, lanes] for i in range(3))
    top_o, total_o, mixed_o = (other_ref[i : i + 1, swapped] for i in range(3))
    high = jnp.maximum(top, top_o)
    own, other = jnp.exp2(top - high), jnp.exp2(top_o - high)
    inverse = 1.0 / (total * own + total_o * other)
    delta = (mixed * own + mixed_o * other) * inverse
    fade = jnp.exp2(stat_ref[0:1, lanes] - high) * inverse
    probs = exp_ref[:, lanes] * fade
    return probs, (probs * (dprob_ref[:, lanes] - delta)).astype(jnp.bfloat16)


def half_lanes(b, width):
    return slice(b * width, (b + 1) * width), slice((1 - b) * width, (2 - b) * width)


def block_grads(group, rows, head, refs, qg_refs, dkv_ref, dscore_ref):
    width = group * rows
    dk = dv = None
    for b in range(2):
        lanes, swapped = half_lanes(b, width)
        probs, dscore = half_weights(refs, lanes, swapped)
        dscore_ref[:, lanes] = dscore
        dk_part = dot_nn(dscore, qg_refs[b][0:width, :])
        dv_part = dot_nn(probs.astype(jnp.bfloat16), qg_refs[b][width : 2 * width, :])
        dk = dk_part if dk is None else dk + dk_part
        dv = dv_part if dv is None else dv + dv_part
    dkv_ref[:, 0:head] = (dk * (1.0 / math.sqrt(head))).astype(dkv_ref.dtype)
    dkv_ref[:, head : 2 * head] = dv.astype(dkv_ref.dtype)


def half_query_grad(group, rows, head, kv_refs, dscores, dq_ref):
    dq = None
    for kv_ref, dscore in zip(kv_refs, dscores):
        part = dot_tn(kv_ref[0:rows, :], dscore)
        dq = part if dq is None else dq + part
    for h in range(group):
        piece = jnp.transpose(dq[:, h * rows : (h + 1) * rows]) * (1.0 / math.sqrt(head))
        dq_ref[:, h * head : (h + 1) * head] = piece.astype(dq_ref.dtype)


def far_grad_kernel(group, rows, head, *refs):
    block_grads(group, rows, head, refs[0:5], refs[5:7], refs[7], refs[8])


def other_query_grad_kernel(blocks, group, rows, head, *refs):
    lanes, swapped = half_lanes(1, group * rows)
    kv_refs = refs[5 : 5 + blocks]
    near = half_weights(refs[0:5], lanes, swapped)[1]
    far = [ref[:, lanes] for ref in refs[5 + blocks : 4 + 2 * blocks]]
    half_query_grad(group, rows, head, kv_refs, [near] + far, refs[4 + 2 * blocks])


def near_grad_kernel(blocks, group, rows, head, *refs):
    lanes = slice(0, group * rows)
    kv_refs = refs[7 : 7 + blocks]
    dkv_ref, dq_ref, dscore_ref = refs[6 + 2 * blocks :]
    block_grads(group, rows, head, refs[0:5], refs[5:7], dkv_ref, dscore_ref)
    dscores = [dscore_ref[:, lanes]] + [ref[:, lanes] for ref in refs[7 + blocks : 6 + 2 * blocks]]
    half_query_grad(group, rows, head, kv_refs, dscores, dq_ref)


def params():
    return pltpu.CompilerParams(vmem_limit_bytes=VMEM_GRANT)


def per_device(queries, keys, values, out_grad, stretch_ids, stash_slot):
    rows, head = keys.shape[2:]
    group = queries.shape[3] // head
    width = group * rows
    count = lax.axis_size("ctx")
    blocks = count // 2
    sections = lax.axis_size("section")

    in_smem = pl.BlockSpec(memory_space=pltpu.SMEM)
    kv = pl.pallas_call(
        fetch_kv_kernel,
        out_shape=jax.ShapeDtypeStruct((2 * rows + ID_ROWS, head), jnp.bfloat16),
        in_specs=[in_smem] + [hbm_spec()] * 3,
        out_specs=vmem_spec(),
        scratch_shapes=[pltpu.SMEM(stretch_ids.shape, jnp.int32), pltpu.SemaphoreType.DMA((3,))],
        compiler_params=params(),
        name="fetch_kv",
    )(stash_slot, in_hbm(stretch_ids), in_hbm(keys), in_hbm(values))
    qg = pl.pallas_call(
        fetch_qg_kernel,
        out_shape=jax.ShapeDtypeStruct((2 * width + ID_ROWS, head), jnp.bfloat16),
        in_specs=[in_smem] + [hbm_spec()] * 2 + [vmem_spec()],
        out_specs=vmem_spec(),
        scratch_shapes=[pltpu.SemaphoreType.DMA((2 * group,))],
        compiler_params=params(),
        name="fetch_qg",
    )(stash_slot, in_hbm(queries), in_hbm(out_grad), kv)

    steps = send_order(count)
    arrivals = arrival_order(count)
    kv_blocks = {0: kv}
    for j in steps:
        kv_blocks[j] = chip_send(kv, count, j)
    qg_other = partner_swap(qg, count)

    square = jax.ShapeDtypeStruct((rows, 2 * width), jnp.float32)
    lines = jax.ShapeDtypeStruct((8, 2 * width), jnp.float32)
    scored = {}
    for j in [0] + arrivals:
        last = j == arrivals[-1]
        earlier = [scored[i][2] for i in scored] if last else []
        scored[j] = pl.pallas_call(
            functools.partial(score_kernel, group, rows, head, len(earlier)),
            out_shape=(square, square, lines) + ((lines,) if last else ()),
            in_specs=[vmem_spec()] * (3 + len(earlier)),
            out_specs=(vmem_spec(),) * (4 if last else 3),
            compiler_params=params(),
        )(qg, qg_other, kv_blocks[j], *earlier)
    merged = scored[arrivals[-1]][3]
    merged_other = partner_swap(merged, count)

    dkv_shape = jax.ShapeDtypeStruct((rows, 2 * head), jnp.bfloat16)
    half_square = jax.ShapeDtypeStruct((rows, 2 * width), jnp.bfloat16)
    returned, dscores = {}, {}
    for j in steps:
        dkv_part, dscores[j] = pl.pallas_call(
            functools.partial(far_grad_kernel, group, rows, head),
            out_shape=(dkv_shape, half_square),
            in_specs=[vmem_spec()] * 7,
            out_specs=(vmem_spec(),) * 2,
            compiler_params=params(),
        )(*scored[j][0:3], merged, merged_other, qg, qg_other)
        returned[j] = chip_return(dkv_part, count, j)
    near = (*scored[0][0:3], merged, merged_other)
    shared = (kv, *(kv_blocks[j] for j in steps), *(dscores[j] for j in steps))
    dq_other = pl.pallas_call(
        functools.partial(other_query_grad_kernel, blocks, group, rows, head),
        out_shape=jax.ShapeDtypeStruct((rows, group * head), jnp.bfloat16),
        in_specs=[vmem_spec()] * (4 + 2 * blocks),
        out_specs=vmem_spec(),
        compiler_params=params(),
        name="dq_other",
    )(*near, *shared)
    dq_swapped = partner_swap(dq_other, count)
    dkv_own, dq_own = pl.pallas_call(
        functools.partial(near_grad_kernel, blocks, group, rows, head),
        out_shape=(
            jax.ShapeDtypeStruct((rows, 2 * head), jnp.float32),
            jax.ShapeDtypeStruct((rows, group * head), jnp.float32),
        ),
        in_specs=[vmem_spec()] * (6 + 2 * blocks),
        out_specs=(vmem_spec(),) * 2,
        scratch_shapes=[pltpu.VMEM((rows, 2 * width), jnp.bfloat16)],
        compiler_params=params(),
        name="grads0",
    )(*near, qg, qg_other, *shared)
    back = [(i, (i - 1) % sections) for i in range(sections)]
    dq = (dq_own + dq_swapped.astype(jnp.float32)).astype(jnp.bfloat16)
    dq_message = lax.ppermute(dq, "section", back)
    dkv = dkv_own
    for j in steps:
        dkv = dkv + returned[j].astype(jnp.float32)
    dkv_message = lax.ppermute(dkv.astype(jnp.bfloat16), "section", back)
    out_shape = jax.ShapeDtypeStruct((1, rows, width // rows * head + 2 * head), jnp.bfloat16)
    filled = pl.pallas_call(
        write_dq_kernel,
        out_shape=out_shape,
        in_specs=[vmem_spec()],
        out_specs=hbm_spec(),
        scratch_shapes=[pltpu.SemaphoreType.DMA],
        compiler_params=params(),
        name="write_dq",
    )(dq_message)
    return pl.pallas_call(
        write_dkv_kernel,
        out_shape=out_shape,
        in_specs=[hbm_spec(), vmem_spec()],
        out_specs=hbm_spec(),
        scratch_shapes=[pltpu.SemaphoreType.DMA],
        input_output_aliases={0: 0},
        compiler_params=params(),
        name="write_dkv",
    )(filled, dkv_message)


def send_order(count):
    return list(reversed(range(1, count // 2)))


def arrival_order(count):
    half = count // 4
    return [j for j in send_order(count) if j != half] + [half]


def solution(mesh):
    in_specs = (
        P("section", None, "ctx", None),
        P("section", None, "ctx", None),
        P("section", None, "ctx", None),
        P("section", "ctx", None),
        P("ctx"),
        P("section"),
    )
    out_specs = P("section", "ctx", None)

    return jax.shard_map(
        per_device, mesh=mesh, in_specs=in_specs, out_specs=out_specs, check_vma=False
    )
```

```python
import functools
import math

import jax
import jax.numpy as jnp
from jax import lax
from jax.experimental import pallas as pl
from jax.experimental.pallas import tpu as pltpu
from jax.sharding import PartitionSpec as P


MASKED = -1e30
FLOOR = -1e29
ID_ROWS = 8
LOG2E = 1.4426950408889634
VMEM_GRANT = 8 * 1024 * 1024


def vmem_spec():
    return pl.BlockSpec(memory_space=pltpu.VMEM)


def in_hbm(value):
    return pltpu.with_memory_space_constraint(value, pltpu.HBM)


def hbm_spec():
    return pl.BlockSpec(memory_space=pltpu.HBM)


def partner_swap(value, count):
    return lax.ppermute(value, "ctx", [(i, i ^ 1) for i in range(count)])


def chip_pairs(count, step):
    chips = count // 2
    if chips & (chips - 1) == 0:
        target = [z ^ step for z in range(chips)]
    else:
        target = [(z + step) % chips for z in range(chips)]
    return [(2 * z + k, 2 * target[z] + k) for z in range(chips) for k in range(2)]


def chip_send(value, count, step):
    return lax.ppermute(value, "ctx", chip_pairs(count, step))


def chip_return(value, count, step):
    return lax.ppermute(value, "ctx", [(b, a) for a, b in chip_pairs(count, step)])


def id_block(ids_ref, head):
    row = lax.broadcasted_iota(jnp.int32, (ID_ROWS, head), 0)
    chosen = jnp.where(row < ID_ROWS // 2, ids_ref[0], ids_ref[1])
    return chosen.astype(jnp.float32).astype(jnp.bfloat16)


def fetch_kv_kernel(slot_ref, ids_ref, key_ref, value_ref, kv_ref, ids, sems):
    rows, head = key_ref.shape[2:]
    slot = slot_ref[0]
    copies = [
        pltpu.make_async_copy(key_ref.at[0, slot], kv_ref.at[0:rows], sems.at[0]),
        pltpu.make_async_copy(value_ref.at[0, slot], kv_ref.at[rows : 2 * rows], sems.at[1]),
    ]
    ids_copy = pltpu.make_async_copy(ids_ref, ids, sems.at[2])
    ids_copy.start()
    for copy in copies:
        copy.start()
    ids_copy.wait()
    kv_ref[2 * rows : 2 * rows + ID_ROWS, :] = id_block(ids, head)
    for copy in copies:
        copy.wait()


def fetch_qg_kernel(slot_ref, query_ref, grad_ref, kv_ref, qg_ref, sems):
    rows, width = query_ref.shape[2:]
    head = kv_ref.shape[1]
    group = width // head
    slot = slot_ref[0]
    copies = []
    for h in range(group):
        cols = slice(h * head, (h + 1) * head)
        query_to = qg_ref.at[h * rows : (h + 1) * rows]
        grad_to = qg_ref.at[(group + h) * rows : (group + h + 1) * rows]
        copies.append(
            pltpu.make_async_copy(query_ref.at[0, slot, :, cols], query_to, sems.at[2 * h])
        )
        copies.append(pltpu.make_async_copy(grad_ref.at[0, :, cols], grad_to, sems.at[2 * h + 1]))
    for copy in copies:
        copy.start()
    last = 2 * group * rows
    qg_ref[last : last + ID_ROWS, :] = kv_ref[2 * rows : 2 * rows + ID_ROWS, :]
    for copy in copies:
        copy.wait()


def write_dq_kernel(dq_ref, out_ref, sem):
    copy = pltpu.make_async_copy(dq_ref, out_ref.at[0, :, 0 : dq_ref.shape[1]], sem)
    copy.start()
    copy.wait()


def write_dkv_kernel(filled_ref, dkv_ref, out_ref, sem):
    start = out_ref.shape[2] - dkv_ref.shape[1]
    copy = pltpu.make_async_copy(dkv_ref, out_ref.at[0, :, start : out_ref.shape[2]], sem)
    copy.start()
    copy.wait()


def id_lines(ref, start, width):
    half = ID_ROWS // 2
    lines = ref[start : start + ID_ROWS, 0:width].astype(jnp.float32)
    return lines[0:1], lines[half : half + 1]


def lane_positions(qg_ref, group, rows, head):
    stretch = rows // 2
    first, second = id_lines(qg_ref, 2 * group * rows, head)
    lane = lax.broadcasted_iota(jnp.int32, (1, rows), 1)
    base = jnp.where(lane < stretch, first, second) * stretch
    offset = jnp.where(lane < stretch, lane, lane - stretch).astype(jnp.float32)
    one_head = base + offset
    return jnp.concatenate([one_head] * group, axis=1)


def dot_nt(a, b):
    return lax.dot_general(a, b, (((1,), (1,)), ((), ())), preferred_element_type=jnp.float32)


def dot_nn(a, b):
    return lax.dot_general(a, b, (((1,), (0,)), ((), ())), preferred_element_type=jnp.float32)


def dot_tn(a, b):
    return lax.dot_general(a, b, (((0,), (0,)), ((), ())), preferred_element_type=jnp.float32)


def score_kernel(group, rows, head, earlier, *refs):
    qg_refs, kv_ref = refs[0:2], refs[2]
    earlier_refs = refs[3 : 3 + earlier]
    exp_ref, dprob_ref, stat_ref = refs[3 + earlier : 6 + earlier]
    width = group * rows
    stretch = rows // 2
    scale = LOG2E / math.sqrt(head)
    in_stretch = lax.broadcasted_iota(jnp.int32, (stretch, 1), 0).astype(jnp.float32)
    ids = id_lines(kv_ref, 2 * rows, head)
    key, value = kv_ref[0:rows, :], kv_ref[rows : 2 * rows, :]
    for b in range(2):
        lanes = slice(b * width, (b + 1) * width)
        place = lane_positions(qg_refs[b], group, rows, head)
        query = qg_refs[b][0:width, :]
        grad = qg_refs[b][width : 2 * width, :]
        scores = dot_nt(key, query) * scale
        dprob = dot_nt(value, grad)
        pieces = []
        for part in range(2):
            limit = place - stretch * jnp.concatenate([ids[part]] * group, axis=1)
            piece = scores[part * stretch : (part + 1) * stretch]
            pieces.append(jnp.where(in_stretch <= limit, piece, MASKED))
        scores = jnp.concatenate(pieces, axis=0)
        top = jnp.maximum(jnp.max(scores, axis=0, keepdims=True), FLOOR)
        raised = jnp.exp2(scores - top)
        exp_ref[:, lanes] = raised
        dprob_ref[:, lanes] = dprob
        stat_ref[0:1, lanes] = top
        stat_ref[1:2, lanes] = jnp.sum(raised, axis=0, keepdims=True)
        stat_ref[2:3, lanes] = jnp.sum(raised * dprob, axis=0, keepdims=True)
        stat_ref[3:8, lanes] = jnp.zeros((5, width), jnp.float32)
    if earlier:
        merged_ref = refs[6 + earlier]
        parts = [ref[...] for ref in earlier_refs] + [stat_ref[...]]
        top = functools.reduce(jnp.maximum, [part[0:1] for part in parts])
        fades = [jnp.exp2(part[0:1] - top) for part in parts]
        merged_ref[0:1, :] = top
        merged_ref[1:2, :] = sum(part[1:2] * fade for part, fade in zip(parts, fades))
        merged_ref[2:3, :] = sum(part[2:3] * fade for part, fade in zip(parts, fades))
        merged_ref[3:8, :] = jnp.zeros((5, 2 * width), jnp.float32)


def half_weights(refs, lanes, swapped):
    exp_ref, dprob_ref, stat_ref, merged_ref, other_ref = refs
    top, total, mixed = (merged_ref[i : i + 1, lanes] for i in range(3))
    top_o, total_o, mixed_o = (other_ref[i : i + 1, swapped] for i in range(3))
    high = jnp.maximum(top, top_o)
    own, other = jnp.exp2(top - high), jnp.exp2(top_o - high)
    inverse = 1.0 / (total * own + total_o * other)
    delta = (mixed * own + mixed_o * other) * inverse
    fade = jnp.exp2(stat_ref[0:1, lanes] - high) * inverse
    probs = exp_ref[:, lanes] * fade
    return probs, (probs * (dprob_ref[:, lanes] - delta)).astype(jnp.bfloat16)


def half_lanes(b, width):
    return slice(b * width, (b + 1) * width), slice((1 - b) * width, (2 - b) * width)


def block_grads(group, rows, head, refs, qg_refs, dkv_ref, dscore_ref):
    width = group * rows
    dk = dv = None
    for b in range(2):
        lanes, swapped = half_lanes(b, width)
        probs, dscore = half_weights(refs, lanes, swapped)
        dscore_ref[:, lanes] = dscore
        dk_part = dot_nn(dscore, qg_refs[b][0:width, :])
        dv_part = dot_nn(probs.astype(jnp.bfloat16), qg_refs[b][width : 2 * width, :])
        dk = dk_part if dk is None else dk + dk_part
        dv = dv_part if dv is None else dv + dv_part
    dkv_ref[:, 0:head] = (dk * (1.0 / math.sqrt(head))).astype(dkv_ref.dtype)
    dkv_ref[:, head : 2 * head] = dv.astype(dkv_ref.dtype)


def half_query_grad(group, rows, head, kv_refs, dscores, dq_ref):
    dq = None
    for kv_ref, dscore in zip(kv_refs, dscores):
        part = dot_tn(kv_ref[0:rows, :], dscore)
        dq = part if dq is None else dq + part
    for h in range(group):
        piece = jnp.transpose(dq[:, h * rows : (h + 1) * rows]) * (1.0 / math.sqrt(head))
        dq_ref[:, h * head : (h + 1) * head] = piece.astype(dq_ref.dtype)


def far_grad_kernel(group, rows, head, span, *refs):
    shared = refs[3 * span : 3 * span + 2]
    qg_refs = refs[3 * span + 2 : 3 * span + 4]
    outs = refs[3 * span + 4 :]
    for i in range(span):
        own = refs[3 * i : 3 * i + 3]
        block_grads(group, rows, head, (*own, *shared), qg_refs, outs[2 * i], outs[2 * i + 1])


def other_query_grad_kernel(blocks, group, rows, head, *refs):
    lanes, swapped = half_lanes(1, group * rows)
    kv_refs = refs[5 : 5 + blocks]
    near = half_weights(refs[0:5], lanes, swapped)[1]
    far = [ref[:, lanes] for ref in refs[5 + blocks : 4 + 2 * blocks]]
    half_query_grad(group, rows, head, kv_refs, [near] + far, refs[4 + 2 * blocks])


def near_grad_kernel(blocks, group, rows, head, *refs):
    lanes = slice(0, group * rows)
    kv_refs = refs[7 : 7 + blocks]
    dkv_ref, dq_ref, dscore_ref = refs[6 + 2 * blocks :]
    block_grads(group, rows, head, refs[0:5], refs[5:7], dkv_ref, dscore_ref)
    dscores = [dscore_ref[:, lanes]] + [ref[:, lanes] for ref in refs[7 + blocks : 6 + 2 * blocks]]
    half_query_grad(group, rows, head, kv_refs, dscores, dq_ref)


def params():
    return pltpu.CompilerParams(vmem_limit_bytes=VMEM_GRANT)


def per_device(queries, keys, values, out_grad, stretch_ids, stash_slot):
    rows, head = keys.shape[2:]
    group = queries.shape[3] // head
    width = group * rows
    count = lax.axis_size("ctx")
    blocks = count // 2
    sections = lax.axis_size("section")

    in_smem = pl.BlockSpec(memory_space=pltpu.SMEM)
    kv = pl.pallas_call(
        fetch_kv_kernel,
        out_shape=jax.ShapeDtypeStruct((2 * rows + ID_ROWS, head), jnp.bfloat16),
        in_specs=[in_smem] + [hbm_spec()] * 3,
        out_specs=vmem_spec(),
        scratch_shapes=[pltpu.SMEM(stretch_ids.shape, jnp.int32), pltpu.SemaphoreType.DMA((3,))],
        compiler_params=params(),
        name="fetch_kv",
    )(stash_slot, in_hbm(stretch_ids), in_hbm(keys), in_hbm(values))
    qg = pl.pallas_call(
        fetch_qg_kernel,
        out_shape=jax.ShapeDtypeStruct((2 * width + ID_ROWS, head), jnp.bfloat16),
        in_specs=[in_smem] + [hbm_spec()] * 2 + [vmem_spec()],
        out_specs=vmem_spec(),
        scratch_shapes=[pltpu.SemaphoreType.DMA((2 * group,))],
        compiler_params=params(),
        name="fetch_qg",
    )(stash_slot, in_hbm(queries), in_hbm(out_grad), kv)

    steps = send_order(count)
    arrivals = arrival_order(count)
    kv_blocks = {0: kv}
    for j in steps:
        kv_blocks[j] = chip_send(kv, count, j)
    qg_other = partner_swap(qg, count)

    square = jax.ShapeDtypeStruct((rows, 2 * width), jnp.float32)
    lines = jax.ShapeDtypeStruct((8, 2 * width), jnp.float32)
    scored = {}
    for j in [0] + arrivals:
        last = j == arrivals[-1]
        earlier = [scored[i][2] for i in scored] if last else []
        scored[j] = pl.pallas_call(
            functools.partial(score_kernel, group, rows, head, len(earlier)),
            out_shape=(square, square, lines) + ((lines,) if last else ()),
            in_specs=[vmem_spec()] * (3 + len(earlier)),
            out_specs=(vmem_spec(),) * (4 if last else 3),
            compiler_params=params(),
        )(qg, qg_other, kv_blocks[j], *earlier)
    merged = scored[arrivals[-1]][3]
    merged_other = partner_swap(merged, count)

    dkv_shape = jax.ShapeDtypeStruct((rows, 2 * head), jnp.bfloat16)
    half_square = jax.ShapeDtypeStruct((rows, 2 * width), jnp.bfloat16)
    returned, dscores = {}, {}
    for part in grad_parts(count):
        results = pl.pallas_call(
            functools.partial(far_grad_kernel, group, rows, head, len(part)),
            out_shape=(dkv_shape, half_square) * len(part),
            in_specs=[vmem_spec()] * (3 * len(part) + 4),
            out_specs=(vmem_spec(),) * (2 * len(part)),
            compiler_params=params(),
        )(*(x for j in part for x in scored[j][0:3]), merged, merged_other, qg, qg_other)
        for i, j in enumerate(part):
            dscores[j] = results[2 * i + 1]
            returned[j] = chip_return(results[2 * i], count, j)
    near = (*scored[0][0:3], merged, merged_other)
    shared = (kv, *(kv_blocks[j] for j in steps), *(dscores[j] for j in steps))
    dq_other = pl.pallas_call(
        functools.partial(other_query_grad_kernel, blocks, group, rows, head),
        out_shape=jax.ShapeDtypeStruct((rows, group * head), jnp.bfloat16),
        in_specs=[vmem_spec()] * (4 + 2 * blocks),
        out_specs=vmem_spec(),
        compiler_params=params(),
        name="dq_other",
    )(*near, *shared)
    dq_swapped = partner_swap(dq_other, count)
    dkv_own, dq_own = pl.pallas_call(
        functools.partial(near_grad_kernel, blocks, group, rows, head),
        out_shape=(
            jax.ShapeDtypeStruct((rows, 2 * head), jnp.float32),
            jax.ShapeDtypeStruct((rows, group * head), jnp.float32),
        ),
        in_specs=[vmem_spec()] * (6 + 2 * blocks),
        out_specs=(vmem_spec(),) * 2,
        scratch_shapes=[pltpu.VMEM((rows, 2 * width), jnp.bfloat16)],
        compiler_params=params(),
        name="grads0",
    )(*near, qg, qg_other, *shared)
    back = [(i, (i - 1) % sections) for i in range(sections)]
    dq = (dq_own + dq_swapped.astype(jnp.float32)).astype(jnp.bfloat16)
    dq_message = lax.ppermute(dq, "section", back)
    dkv = dkv_own
    for j in steps:
        dkv = dkv + returned[j].astype(jnp.float32)
    dkv_message = lax.ppermute(dkv.astype(jnp.bfloat16), "section", back)
    out_shape = jax.ShapeDtypeStruct((1, rows, width // rows * head + 2 * head), jnp.bfloat16)
    filled = pl.pallas_call(
        write_dq_kernel,
        out_shape=out_shape,
        in_specs=[vmem_spec()],
        out_specs=hbm_spec(),
        scratch_shapes=[pltpu.SemaphoreType.DMA],
        compiler_params=params(),
        name="write_dq",
    )(dq_message)
    return pl.pallas_call(
        write_dkv_kernel,
        out_shape=out_shape,
        in_specs=[hbm_spec(), vmem_spec()],
        out_specs=hbm_spec(),
        scratch_shapes=[pltpu.SemaphoreType.DMA],
        input_output_aliases={0: 0},
        compiler_params=params(),
        name="write_dkv",
    )(filled, dkv_message)


def send_order(count):
    return list(reversed(range(1, count // 2)))


def arrival_order(count):
    half = count // 4
    return [j for j in send_order(count) if j != half] + [half]


def grad_parts(count):
    steps = send_order(count)
    return [steps[0:1], steps[1:]]


def solution(mesh):
    in_specs = (
        P("section", None, "ctx", None),
        P("section", None, "ctx", None),
        P("section", None, "ctx", None),
        P("section", "ctx", None),
        P("ctx"),
        P("section"),
    )
    out_specs = P("section", "ctx", None)

    return jax.shard_map(
        per_device, mesh=mesh, in_specs=in_specs, out_specs=out_specs, check_vma=False
    )
```

```python
import functools
import math

import jax
import jax.numpy as jnp
from jax import lax
from jax.experimental import pallas as pl
from jax.experimental.pallas import tpu as pltpu
from jax.sharding import PartitionSpec as P


MASKED = -1e30
FLOOR = -1e29
ID_ROWS = 8
LOG2E = 1.4426950408889634
VMEM_GRANT = 8 * 1024 * 1024


def vmem_spec():
    return pl.BlockSpec(memory_space=pltpu.VMEM)


def in_hbm(value):
    return pltpu.with_memory_space_constraint(value, pltpu.HBM)


def hbm_spec():
    return pl.BlockSpec(memory_space=pltpu.HBM)


def partner_swap(value, count):
    return lax.ppermute(value, "ctx", [(i, i ^ 1) for i in range(count)])


def chip_pairs(count, step):
    chips = count // 2
    if chips & (chips - 1) == 0:
        target = [z ^ step for z in range(chips)]
    else:
        target = [(z + step) % chips for z in range(chips)]
    return [(2 * z + k, 2 * target[z] + k) for z in range(chips) for k in range(2)]


def chip_send(value, count, step):
    return lax.ppermute(value, "ctx", chip_pairs(count, step))


def chip_return(value, count, step):
    return lax.ppermute(value, "ctx", [(b, a) for a, b in chip_pairs(count, step)])


def id_block(ids_ref, head):
    row = lax.broadcasted_iota(jnp.int32, (ID_ROWS, head), 0)
    chosen = jnp.where(row < ID_ROWS // 2, ids_ref[0], ids_ref[1])
    return chosen.astype(jnp.float32).astype(jnp.bfloat16)


def fetch_kv_kernel(slot_ref, ids_ref, key_ref, value_ref, kv_ref, ids, sems):
    rows, head = key_ref.shape[2:]
    slot = slot_ref[0]
    copies = [
        pltpu.make_async_copy(key_ref.at[0, slot], kv_ref.at[0:rows], sems.at[0]),
        pltpu.make_async_copy(value_ref.at[0, slot], kv_ref.at[rows : 2 * rows], sems.at[1]),
    ]
    ids_copy = pltpu.make_async_copy(ids_ref, ids, sems.at[2])
    ids_copy.start()
    for copy in copies:
        copy.start()
    ids_copy.wait()
    kv_ref[2 * rows : 2 * rows + ID_ROWS, :] = id_block(ids, head)
    for copy in copies:
        copy.wait()


def fetch_qg_kernel(slot_ref, query_ref, grad_ref, kv_ref, qg_ref, sems):
    rows, width = query_ref.shape[2:]
    head = kv_ref.shape[1]
    group = width // head
    slot = slot_ref[0]
    copies = []
    for h in range(group):
        cols = slice(h * head, (h + 1) * head)
        query_to = qg_ref.at[h * rows : (h + 1) * rows]
        grad_to = qg_ref.at[(group + h) * rows : (group + h + 1) * rows]
        copies.append(
            pltpu.make_async_copy(query_ref.at[0, slot, :, cols], query_to, sems.at[2 * h])
        )
        copies.append(pltpu.make_async_copy(grad_ref.at[0, :, cols], grad_to, sems.at[2 * h + 1]))
    for copy in copies:
        copy.start()
    last = 2 * group * rows
    qg_ref[last : last + ID_ROWS, :] = kv_ref[2 * rows : 2 * rows + ID_ROWS, :]
    for copy in copies:
        copy.wait()


def write_dq_kernel(dq_ref, out_ref, sem):
    copy = pltpu.make_async_copy(dq_ref, out_ref.at[0, :, 0 : dq_ref.shape[1]], sem)
    copy.start()
    copy.wait()


def write_dkv_kernel(filled_ref, dkv_ref, out_ref, sem):
    start = out_ref.shape[2] - dkv_ref.shape[1]
    copy = pltpu.make_async_copy(dkv_ref, out_ref.at[0, :, start : out_ref.shape[2]], sem)
    copy.start()
    copy.wait()


def id_lines(ref, start, width):
    half = ID_ROWS // 2
    lines = ref[start : start + ID_ROWS, 0:width].astype(jnp.float32)
    return lines[0:1], lines[half : half + 1]


def lane_positions(qg_ref, group, rows, head):
    stretch = rows // 2
    first, second = id_lines(qg_ref, 2 * group * rows, head)
    lane = lax.broadcasted_iota(jnp.int32, (1, rows), 1)
    base = jnp.where(lane < stretch, first, second) * stretch
    offset = jnp.where(lane < stretch, lane, lane - stretch).astype(jnp.float32)
    one_head = base + offset
    return jnp.concatenate([one_head] * group, axis=1)


def dot_nt(a, b):
    return lax.dot_general(a, b, (((1,), (1,)), ((), ())), preferred_element_type=jnp.float32)


def dot_nn(a, b):
    return lax.dot_general(a, b, (((1,), (0,)), ((), ())), preferred_element_type=jnp.float32)


def dot_tn(a, b):
    return lax.dot_general(a, b, (((0,), (0,)), ((), ())), preferred_element_type=jnp.float32)


def score_kernel(group, rows, head, earlier, *refs):
    qg_refs, kv_ref = refs[0:2], refs[2]
    earlier_refs = refs[3 : 3 + earlier]
    exp_ref, dprob_ref, stat_ref = refs[3 + earlier : 6 + earlier]
    width = group * rows
    stretch = rows // 2
    scale = LOG2E / math.sqrt(head)
    in_stretch = lax.broadcasted_iota(jnp.int32, (stretch, 1), 0).astype(jnp.float32)
    ids = id_lines(kv_ref, 2 * rows, head)
    key, value = kv_ref[0:rows, :], kv_ref[rows : 2 * rows, :]
    for b in range(2):
        lanes = slice(b * width, (b + 1) * width)
        place = lane_positions(qg_refs[b], group, rows, head)
        query = qg_refs[b][0:width, :]
        grad = qg_refs[b][width : 2 * width, :]
        scores = dot_nt(key, query) * scale
        dprob = dot_nt(value, grad)
        pieces = []
        for part in range(2):
            limit = place - stretch * jnp.concatenate([ids[part]] * group, axis=1)
            piece = scores[part * stretch : (part + 1) * stretch]
            pieces.append(jnp.where(in_stretch <= limit, piece, MASKED))
        scores = jnp.concatenate(pieces, axis=0)
        top = jnp.maximum(jnp.max(scores, axis=0, keepdims=True), FLOOR)
        raised = jnp.exp2(scores - top)
        exp_ref[:, lanes] = raised
        dprob_ref[:, lanes] = dprob
        stat_ref[0:1, lanes] = top
        stat_ref[1:2, lanes] = jnp.sum(raised, axis=0, keepdims=True)
        stat_ref[2:3, lanes] = jnp.sum(raised * dprob, axis=0, keepdims=True)
        stat_ref[3:8, lanes] = jnp.zeros((5, width), jnp.float32)
    if earlier:
        merged_ref = refs[6 + earlier]
        parts = [ref[0:3, :] for ref in earlier_refs] + [stat_ref[0:3, :]]
        top = functools.reduce(jnp.maximum, [part[0:1] for part in parts])
        fades = [jnp.exp2(part[0:1] - top) for part in parts]
        merged_ref[0:1, :] = top
        merged_ref[1:2, :] = sum(part[1:2] * fade for part, fade in zip(parts, fades))
        merged_ref[2:3, :] = sum(part[2:3] * fade for part, fade in zip(parts, fades))
        merged_ref[3:8, :] = jnp.zeros((5, 2 * width), jnp.float32)


def half_weights(refs, lanes, swapped):
    exp_ref, dprob_ref, stat_ref, merged_ref, other_ref = refs
    top, total, mixed = (merged_ref[i : i + 1, lanes] for i in range(3))
    top_o, total_o, mixed_o = (other_ref[i : i + 1, swapped] for i in range(3))
    high = jnp.maximum(top, top_o)
    own, other = jnp.exp2(top - high), jnp.exp2(top_o - high)
    inverse = 1.0 / (total * own + total_o * other)
    delta = (mixed * own + mixed_o * other) * inverse
    fade = jnp.exp2(stat_ref[0:1, lanes] - high) * inverse
    probs = exp_ref[:, lanes] * fade
    return probs, (probs * (dprob_ref[:, lanes] - delta)).astype(jnp.bfloat16)


def half_lanes(b, width):
    return slice(b * width, (b + 1) * width), slice((1 - b) * width, (2 - b) * width)


def block_grads(group, rows, head, refs, qg_refs, dkv_ref, dscore_ref):
    width = group * rows
    dk = dv = None
    for b in range(2):
        lanes, swapped = half_lanes(b, width)
        probs, dscore = half_weights(refs, lanes, swapped)
        dscore_ref[:, lanes] = dscore
        dk_part = dot_nn(dscore, qg_refs[b][0:width, :])
        dv_part = dot_nn(probs.astype(jnp.bfloat16), qg_refs[b][width : 2 * width, :])
        dk = dk_part if dk is None else dk + dk_part
        dv = dv_part if dv is None else dv + dv_part
    dkv_ref[:, 0:head] = (dk * (1.0 / math.sqrt(head))).astype(dkv_ref.dtype)
    dkv_ref[:, head : 2 * head] = dv.astype(dkv_ref.dtype)


def half_query_grad(group, rows, head, kv_refs, dscores, dq_ref):
    dq = None
    for kv_ref, dscore in zip(kv_refs, dscores):
        part = dot_tn(kv_ref[0:rows, :], dscore)
        dq = part if dq is None else dq + part
    for h in range(group):
        piece = jnp.transpose(dq[:, h * rows : (h + 1) * rows]) * (1.0 / math.sqrt(head))
        dq_ref[:, h * head : (h + 1) * head] = piece.astype(dq_ref.dtype)


def far_grad_kernel(group, rows, head, span, *refs):
    shared = refs[3 * span : 3 * span + 2]
    qg_refs = refs[3 * span + 2 : 3 * span + 4]
    outs = refs[3 * span + 4 :]
    for i in range(span):
        own = refs[3 * i : 3 * i + 3]
        block_grads(group, rows, head, (*own, *shared), qg_refs, outs[2 * i], outs[2 * i + 1])


def other_query_grad_kernel(blocks, group, rows, head, *refs):
    lanes, swapped = half_lanes(1, group * rows)
    kv_refs = refs[5 : 5 + blocks]
    near = half_weights(refs[0:5], lanes, swapped)[1]
    far = [ref[:, lanes] for ref in refs[5 + blocks : 4 + 2 * blocks]]
    half_query_grad(group, rows, head, kv_refs, [near] + far, refs[4 + 2 * blocks])


def near_grad_kernel(blocks, group, rows, head, *refs):
    lanes = slice(0, group * rows)
    kv_refs = refs[7 : 7 + blocks]
    dkv_ref, dq_ref, dscore_ref = refs[6 + 2 * blocks :]
    block_grads(group, rows, head, refs[0:5], refs[5:7], dkv_ref, dscore_ref)
    dscores = [dscore_ref[:, lanes]] + [ref[:, lanes] for ref in refs[7 + blocks : 6 + 2 * blocks]]
    half_query_grad(group, rows, head, kv_refs, dscores, dq_ref)


def params():
    return pltpu.CompilerParams(vmem_limit_bytes=VMEM_GRANT)


def per_device(queries, keys, values, out_grad, stretch_ids, stash_slot):
    rows, head = keys.shape[2:]
    group = queries.shape[3] // head
    width = group * rows
    count = lax.axis_size("ctx")
    blocks = count // 2
    sections = lax.axis_size("section")

    in_smem = pl.BlockSpec(memory_space=pltpu.SMEM)
    kv = pl.pallas_call(
        fetch_kv_kernel,
        out_shape=jax.ShapeDtypeStruct((2 * rows + ID_ROWS, head), jnp.bfloat16),
        in_specs=[in_smem] + [hbm_spec()] * 3,
        out_specs=vmem_spec(),
        scratch_shapes=[pltpu.SMEM(stretch_ids.shape, jnp.int32), pltpu.SemaphoreType.DMA((3,))],
        compiler_params=params(),
        name="fetch_kv",
    )(stash_slot, in_hbm(stretch_ids), in_hbm(keys), in_hbm(values))
    qg = pl.pallas_call(
        fetch_qg_kernel,
        out_shape=jax.ShapeDtypeStruct((2 * width + ID_ROWS, head), jnp.bfloat16),
        in_specs=[in_smem] + [hbm_spec()] * 2 + [vmem_spec()],
        out_specs=vmem_spec(),
        scratch_shapes=[pltpu.SemaphoreType.DMA((2 * group,))],
        compiler_params=params(),
        name="fetch_qg",
    )(stash_slot, in_hbm(queries), in_hbm(out_grad), kv)

    steps = return_order(count)
    arrivals = arrival_order(count)
    kv_blocks = {0: kv}
    for j in send_order(count):
        kv_blocks[j] = chip_send(kv, count, j)
    qg_other = partner_swap(qg, count)

    square = jax.ShapeDtypeStruct((rows, 2 * width), jnp.float32)
    lines = jax.ShapeDtypeStruct((8, 2 * width), jnp.float32)
    scored, merged = {}, None
    for j in [0] + arrivals:
        if j == arrivals[-1]:
            earlier = [merged]
        elif j == arrivals[-2]:
            earlier = [scored[i][2] for i in scored]
        else:
            earlier = []
        merging = 1 if earlier else 0
        scored[j] = pl.pallas_call(
            functools.partial(score_kernel, group, rows, head, len(earlier)),
            out_shape=(square, square, lines) + (lines,) * merging,
            in_specs=[vmem_spec()] * (3 + len(earlier)),
            out_specs=(vmem_spec(),) * (3 + merging),
            compiler_params=params(),
        )(qg, qg_other, kv_blocks[j], *earlier)
        if earlier:
            merged = scored[j][3]
    merged_other = partner_swap(merged, count)

    dkv_shape = jax.ShapeDtypeStruct((rows, 2 * head), jnp.bfloat16)
    half_square = jax.ShapeDtypeStruct((rows, 2 * width), jnp.bfloat16)
    returned, dscores = {}, {}
    for part in grad_parts(count):
        results = pl.pallas_call(
            functools.partial(far_grad_kernel, group, rows, head, len(part)),
            out_shape=(dkv_shape, half_square) * len(part),
            in_specs=[vmem_spec()] * (3 * len(part) + 4),
            out_specs=(vmem_spec(),) * (2 * len(part)),
            compiler_params=params(),
        )(*(x for j in part for x in scored[j][0:3]), merged, merged_other, qg, qg_other)
        for i, j in enumerate(part):
            dscores[j] = results[2 * i + 1]
            returned[j] = chip_return(results[2 * i], count, j)
    near = (*scored[0][0:3], merged, merged_other)
    shared = (kv, *(kv_blocks[j] for j in steps), *(dscores[j] for j in steps))
    dq_other = pl.pallas_call(
        functools.partial(other_query_grad_kernel, blocks, group, rows, head),
        out_shape=jax.ShapeDtypeStruct((rows, group * head), jnp.bfloat16),
        in_specs=[vmem_spec()] * (4 + 2 * blocks),
        out_specs=vmem_spec(),
        compiler_params=params(),
        name="dq_other",
    )(*near, *shared)
    dq_swapped = partner_swap(dq_other, count)
    dkv_own, dq_own = pl.pallas_call(
        functools.partial(near_grad_kernel, blocks, group, rows, head),
        out_shape=(
            jax.ShapeDtypeStruct((rows, 2 * head), jnp.float32),
            jax.ShapeDtypeStruct((rows, group * head), jnp.float32),
        ),
        in_specs=[vmem_spec()] * (6 + 2 * blocks),
        out_specs=(vmem_spec(),) * 2,
        scratch_shapes=[pltpu.VMEM((rows, 2 * width), jnp.bfloat16)],
        compiler_params=params(),
        name="grads0",
    )(*near, qg, qg_other, *shared)
    back = [(i, (i - 1) % sections) for i in range(sections)]
    dq = (dq_own + dq_swapped.astype(jnp.float32)).astype(jnp.bfloat16)
    dq_message = lax.ppermute(dq, "section", back)
    dkv = dkv_own
    for j in steps:
        dkv = dkv + returned[j].astype(jnp.float32)
    dkv_message = lax.ppermute(dkv.astype(jnp.bfloat16), "section", back)
    out_shape = jax.ShapeDtypeStruct((1, rows, width // rows * head + 2 * head), jnp.bfloat16)
    filled = pl.pallas_call(
        write_dq_kernel,
        out_shape=out_shape,
        in_specs=[vmem_spec()],
        out_specs=hbm_spec(),
        scratch_shapes=[pltpu.SemaphoreType.DMA],
        compiler_params=params(),
        name="write_dq",
    )(dq_message)
    return pl.pallas_call(
        write_dkv_kernel,
        out_shape=out_shape,
        in_specs=[hbm_spec(), vmem_spec()],
        out_specs=hbm_spec(),
        scratch_shapes=[pltpu.SemaphoreType.DMA],
        input_output_aliases={0: 0},
        compiler_params=params(),
        name="write_dkv",
    )(filled, dkv_message)


def send_order(count):
    half = count // 4
    return [j for j in reversed(range(1, count // 2)) if j != half] + [half]


def return_order(count):
    return send_order(count)


def arrival_order(count):
    return send_order(count)


def grad_parts(count):
    steps = return_order(count)
    return [steps[0:1], steps[1:]]


def solution(mesh):
    in_specs = (
        P("section", None, "ctx", None),
        P("section", None, "ctx", None),
        P("section", None, "ctx", None),
        P("section", "ctx", None),
        P("ctx"),
        P("section"),
    )
    out_specs = P("section", "ctx", None)

    return jax.shard_map(
        per_device, mesh=mesh, in_specs=in_specs, out_specs=out_specs, check_vma=False
    )
```
